32 devices in a mesh: sub: 16 (over z, y, x), agg: 2 (over core).
Axes of the slice: x: 2, y: 2, z: 4, core: 2. Of those that a mesh axis runs over, the one named last changes fastest.
Arguments:
- block_values: float32 [7, 4, 4, 32768], P(None, None, None, ('sub', 'agg'))
- block_cols: int32 [7, 32768], P(None, ('sub', 'agg')), may hold values from 0 to 32767, as said below
- coarse_rhs: float32 [4, 32768], P(None, ('sub', 'agg'))
- guess: float32 [4, 32768], P(None, ('sub', 'agg')), may hold values from -3 to 3
- bound_low: int32 [1], replicated, may hold values from 20 to 26
- bound_high: int32 [1], replicated, may hold values from 32 to 40
Outputs:
- smoothed: float32 [4, 32768], P(None, ('sub', 'agg'))
- residual: float32 [4, 32768], P(None, ('sub', 'agg'))
- residual_rms: float32 [1], replicated
The draws below stay inside these ranges and needn't reach their ends.
Inputs may be any that keep to these rules, and one draw needn't show every extreme that they name: Block rows form 32768 / 1024 planes of 1024 consecutive rows, in a periodic order. block_cols[0] is the row itself, block_cols[1] a row of the previous plane, block_cols[2] a row of the next plane, block_cols[3] to block_cols[6] rows of the same plane.
All inputs are finite; a program needn't handle non-finite values.
Results may differ from the reference program's by a relative error of at most 0.0001.
Values sent between devices are 32-bit elements; how exact they have to be, the bound alone decides.
A program may use at most 64 MiB of HBM per device.

```python
import jax
import jax.numpy as jnp
from jax import lax

ROWS_DEV = 1024
COMP = 4
NEIGHBORS = 7
STEPS = 4
TOTAL = 32768


def draw_block_values(key, part):
    noise = 0.5 * jax.random.normal(key, (NEIGHBORS, COMP, COMP, TOTAL), jnp.float32)
    identity = jnp.eye(COMP, dtype=jnp.float32)[:, :, None]
    diagonal_block = noise[0] * (1.0 - identity) + 6.0 * identity
    return jnp.concatenate([diagonal_block[None], noise[1:]], axis=0)


def draw_block_cols(key, part):
    planes = TOTAL // ROWS_DEV
    rows_all = jnp.arange(TOTAL, dtype=jnp.int32)
    plane_of = rows_all // ROWS_DEV
    picked = jax.random.randint(key, (6, TOTAL), 0, ROWS_DEV).astype(jnp.int32)
    before = (plane_of - 1) % planes * ROWS_DEV + picked[0]
    after = (plane_of + 1) % planes * ROWS_DEV + picked[1]
    same_plane = plane_of[None, :] * ROWS_DEV + picked[2:]
    return jnp.concatenate([rows_all[None], before[None], after[None], same_plane], axis=0).astype(jnp.int32)


def draw_coarse_rhs(key, part):
    rows_all = jnp.arange(TOTAL, dtype=jnp.float32)
    scale_row = 0.5 + 0.5 * rows_all / TOTAL
    values = jax.random.normal(key, (COMP, TOTAL), jnp.float32)
    return values * scale_row[None, :]


def steps_of(own_key, extent, cuts, least, high):
    loudness = 1.0
    for dim, shards_of in cuts:
        draws = jax.random.uniform(jax.random.fold_in(jax.random.fold_in(own_key, 6), dim), (shards_of,), jnp.float32, least / len(cuts), high / len(cuts))
        loudness = loudness * jnp.repeat(jnp.exp(draws), extent[dim] // shards_of).reshape((-1,) + (1,) * (len(extent) - 1 - dim))
    return loudness


def scatter_about(rng, shape, scale, limit, cuts=(), held_as=jnp.bfloat16):
    array = jax.random.normal(rng, shape, jnp.float32) * scale
    if len(cuts) > 0:
        array = steps_of(rng, shape, cuts, -0.22, 0.18) * array
    return jnp.clip(array, min=-limit, max=limit).astype(held_as)


def setup_inputs(seed: int = 0) -> dict:
    splits = jax.random.split(jax.random.key(seed), 7)
    block_values = draw_block_values(jax.random.fold_in(splits[6], 71), 0)
    block_cols = draw_block_cols(jax.random.fold_in(splits[6], 71), 0)
    coarse_rhs = draw_coarse_rhs(jax.random.fold_in(splits[6], 71), 0)
    guess = scatter_about(splits[3], (COMP, TOTAL), 0.5, 3.0, ((1, 32),), jnp.float32)
    bound_low = jax.random.randint(splits[4], (1,), 20, 27).astype(jnp.int32)
    bound_high = jax.random.randint(splits[5], (1,), 32, 41).astype(jnp.int32)
    return dict(block_values=block_values, block_cols=block_cols, coarse_rhs=coarse_rhs, guess=guess, bound_low=bound_low, bound_high=bound_high)


def apply_blocks(block_values, position, field):
    count = position.shape[0]
    width = position.shape[1]
    taken = jnp.take(field, position.reshape(-1), axis=1).reshape(field.shape[0], count, width)
    result = jnp.zeros((field.shape[0], width), jnp.float32)
    for column in range(field.shape[0]):
        result = result + lax.optimization_barrier(jnp.sum(block_values[:, :, column, :] * taken[column][:, None, :], axis=0))
    return result

def reference(block_values, block_cols, coarse_rhs, guess, bound_low, bound_high):
    lower = bound_low[0].astype(jnp.float32) / 4.0
    upper = bound_high[0].astype(jnp.float32) / 4.0
    centre = (upper + lower) / 2.0
    half_width = (upper - lower) / 2.0
    spread_ratio = centre / half_width
    ratio_prev = 1.0 / spread_ratio
    smoothed = guess
    residual = coarse_rhs - apply_blocks(block_values, block_cols, guess)
    direction = residual / centre
    for step in range(STEPS):
        smoothed = smoothed + direction
        residual = residual - apply_blocks(block_values, block_cols, direction)
        if step + 1 < STEPS:
            ratio_next = 1.0 / (2.0 * spread_ratio - ratio_prev)
            direction = ratio_next * ratio_prev * direction + 2.0 * ratio_next / half_width * residual
            ratio_prev = ratio_next
    total_sq = jnp.sum(residual * residual)
    residual_rms = jnp.sqrt(total_sq / (4.0 * TOTAL) + 1e-06).reshape(1)
    return (smoothed, residual, residual_rms)
```

```python
import functools

import jax
import jax.numpy as jnp
from jax import lax
from jax.experimental import pallas as pl
from jax.experimental.pallas import tpu as pltpu
from jax.sharding import PartitionSpec as P

STEPS = 4
LANES = 128
MESH = pl.DeviceIdType.MESH


def group_size(devices):
    size = 1
    while size * size < devices or devices % size:
        size += 1
    return size


def gather_lanes(rows, index):
    return jnp.take_along_axis(rows, index, axis=1, mode="promise_in_bounds")


def kernel(
    subs, aggs, shape,
    values_hbm, cols_hbm, rhs_hbm, guess_hbm, low_ref, high_ref,
    smoothed_hbm, residual_hbm, rms_ref,
    values, cols, cols_flat, rhs, field, beside, lane_of, tile_of, coef,
    smoothed_out, residual_out, near_sums, far_sums,
    values_sem, load_sem, store_sem, send_sem, recv_sem,
    near_send, near_recv, far_send, far_recv,
):
    blocks, comp, tiles = shape
    devices = subs * aggs
    rows = tiles * LANES
    me = lax.axis_index("sub") * aggs + lax.axis_index("agg")

    def coords(device):
        return (device // aggs, device % aggs)

    following = lax.rem(me + 1, devices)
    previous = lax.rem(me + devices - 1, devices)
    near = group_size(devices)
    far = devices // near
    near_me = lax.rem(me, near)
    near_base = me - near_me
    far_me = me // near
    near_partners = [near_base + lax.rem(near_me + d, near) for d in range(1, near)]
    far_partners = [lax.rem(me + d * near, devices) for d in range(1, far)]

    barrier = pltpu.get_barrier_semaphore()
    partners = [following, previous] + far_partners + near_partners
    for partner in partners:
        pl.semaphore_signal(barrier, inc=1, device_id=coords(partner), device_id_type=MESH)

    load_cols = pltpu.make_async_copy(cols_hbm, cols, load_sem.at[0])
    load_guess = pltpu.make_async_copy(guess_hbm, field.at[0], load_sem.at[1])
    load_rhs = pltpu.make_async_copy(rhs_hbm, rhs, load_sem.at[2])
    load_cols.start()
    load_guess.start()
    own = [0] + list(range(3, blocks))
    per_block = comp * comp * tiles

    def load_values(k):
        part = pl.ds(k * per_block, per_block)
        return pltpu.make_async_copy(values_hbm.at[part], values.at[part], values_sem.at[k])

    for k in own + [1, 2]:
        load_values(k).start()
    load_rhs.start()

    pl.semaphore_wait(barrier, len(partners))

    def send(step, source, way):
        return pltpu.make_async_remote_copy(
            src_ref=source,
            dst_ref=beside.at[step, way],
            send_sem=send_sem.at[step, way],
            recv_sem=recv_sem.at[step, way],
            device_id=coords(following if way == 0 else previous),
            device_id_type=MESH,
        )

    for way in range(2):
        send(0, guess_hbm, way).start()

    low = jnp.full((tiles, LANES), low_ref[0], jnp.int32).astype(jnp.float32) / 4.0
    high = jnp.full((tiles, LANES), high_ref[0], jnp.int32).astype(jnp.float32) / 4.0
    centre = (high + low) / 2.0
    half = (high - low) / 2.0
    spread = centre / half
    ratio = 1.0 / spread
    coef[0, 0] = jnp.zeros((tiles, LANES), jnp.float32)
    coef[0, 1] = 1.0 / centre
    for t in range(1, STEPS):
        ahead = 1.0 / (2.0 * spread - ratio)
        coef[t, 0] = ahead * ratio
        coef[t, 1] = 2.0 * ahead / half
        ratio = ahead

    load_cols.wait()
    for c in range(tiles):
        cols_flat[pl.ds(c * 8, blocks), :] = cols[:, c * LANES:(c + 1) * LANES]
    for k in range(1, blocks):
        plane = {1: previous, 2: following}.get(k, me)
        local = cols_flat[pl.ds(k, tiles, stride=8), :] - plane * rows
        lane_of[k] = local & (LANES - 1)
        tile_of[k] = local >> 7

    def taken(source, k):
        lanes, tile = lane_of[k], tile_of[k]
        out = [None] * comp
        for r in range(tiles):
            here = tile == r
            for j in range(comp):
                row = jnp.broadcast_to(source[pl.ds(r * comp + j, 1), :], (tiles, LANES))
                got = gather_lanes(row, lanes)
                out[j] = got if r == 0 else jnp.where(here, got, out[j])
        return out

    def combine(k, got, total):
        total = list(total)
        for i in range(comp):
            base = (k * comp + i) * comp * tiles
            for j in range(comp):
                total[i] = total[i] - values[pl.ds(base + j, tiles, stride=comp), :] * got[j]
        return total

    def own_part(t, residual):
        source = field.at[t]
        direct = [source[pl.ds(j, tiles, stride=comp), :] for j in range(comp)]
        residual = combine(0, direct, residual)
        for k in own[1:]:
            residual = combine(k, taken(source, k), residual)
        return direct, residual

    def far_part(t, residual):
        for way in range(2):
            send(t, field.at[t], way).wait_recv()
            residual = combine(1 + way, taken(beside.at[t, way], 1 + way), residual)
        return residual

    load_guess.wait()
    load_rhs.wait()
    for k in own + [1, 2]:
        load_values(k).wait()

    def step(t, carry):
        smoothed, residual = carry
        direct, residual = own_part(t, residual)
        smoothed = [s + d for s, d in zip(smoothed, direct)]
        residual = far_part(t, residual)
        for j in range(comp):
            field[t + 1, pl.ds(j, tiles, stride=comp), :] = (
                coef[t, 0] * direct[j] + coef[t, 1] * residual[j]
            )
        for way in range(2):
            send(t + 1, field.at[t + 1], way).start()
        return smoothed, residual

    smoothed = [jnp.zeros((tiles, LANES), jnp.float32) for j in range(comp)]
    residual = [rhs[pl.ds(j, tiles, stride=comp), :] for j in range(comp)]
    smoothed, residual = lax.fori_loop(0, STEPS, step, (smoothed, residual))

    direct, residual = own_part(STEPS, residual)
    for j in range(comp):
        smoothed_out[pl.ds(j, tiles, stride=comp), :] = smoothed[j] + direct[j]
    store_smoothed = pltpu.make_async_copy(smoothed_out, smoothed_hbm, store_sem.at[0])
    store_smoothed.start()
    residual = far_part(STEPS, residual)

    squares = residual[0] * residual[0]
    for j in range(1, comp):
        squares = squares + residual[j] * residual[j]
    partial = jnp.sum(squares, axis=0, keepdims=True)

    def spread_sums(sums, slot, partner, send_sems, recv_sems, d):
        return pltpu.make_async_remote_copy(
            src_ref=sums.at[slot],
            dst_ref=sums.at[slot],
            send_sem=send_sems.at[d],
            recv_sem=recv_sems.at[slot],
            device_id=coords(partner),
            device_id_type=MESH,
        )

    def total_over(partial, sums, size, place, partners, send_sems, recv_sems):
        sums[place] = partial
        for d, partner in enumerate(partners):
            spread_sums(sums, place, partner, send_sems, recv_sems, d).start()

        def finish():
            for d, partner in enumerate(partners):
                slot = lax.rem(place + d + 1, size)
                spread_sums(sums, slot, partner, send_sems, recv_sems, d).wait_recv()
            total = sums[0]
            for slot in range(1, size):
                total = total + sums[slot]
            return total

        return finish

    finish = total_over(partial, near_sums, near, near_me, near_partners, near_send, near_recv)
    for j in range(comp):
        residual_out[pl.ds(j, tiles, stride=comp), :] = residual[j]
    store_residual = pltpu.make_async_copy(residual_out, residual_hbm, store_sem.at[1])
    store_residual.start()
    partial = finish()
    finish = total_over(partial, far_sums, far, far_me, far_partners, far_send, far_recv)
    total = finish()
    count = float(comp * rows * devices)
    rms = jnp.sqrt(jnp.sum(total, axis=1, keepdims=True) / count + 1e-06)
    rms_ref[0] = rms[0, 0]

    for t in range(STEPS + 1):
        for way in range(2):
            send(t, field.at[t], way).wait_send()
    for d, partner in enumerate(near_partners):
        spread_sums(near_sums, near_me, partner, near_send, near_recv, d).wait_send()
    for d, partner in enumerate(far_partners):
        spread_sums(far_sums, far_me, partner, far_send, far_recv, d).wait_send()
    store_smoothed.wait()
    store_residual.wait()


def flat(field, tiles):
    comp = field.shape[-2]
    lead = field.shape[:-2]
    cut = field.reshape(lead + (comp, tiles, LANES))
    return jnp.swapaxes(cut, -3, -2).reshape(-1, LANES)


def unflat(field, comp):
    tiles = field.shape[0] // comp
    return jnp.swapaxes(field.reshape(tiles, comp, LANES), 0, 1).reshape(comp, tiles * LANES)


def shards(subs, aggs, block_values, block_cols, coarse_rhs, guess, bound_low, bound_high):
    blocks, comp, _, rows = block_values.shape
    tiles = rows // LANES
    devices = subs * aggs
    near = group_size(devices)
    far = devices // near
    f32 = jnp.float32
    plane = (tiles * comp, LANES)
    anywhere = pl.BlockSpec(memory_space=pl.ANY)
    scalar = pl.BlockSpec(memory_space=pltpu.SMEM)
    dma = pltpu.SemaphoreType.DMA
    smoothed, residual, rms = pl.pallas_call(
        functools.partial(kernel, subs, aggs, (blocks, comp, tiles)),
        out_shape=(
            jax.ShapeDtypeStruct(plane, f32),
            jax.ShapeDtypeStruct(plane, f32),
            jax.ShapeDtypeStruct((1,), f32),
        ),
        in_specs=[anywhere] * 4 + [scalar] * 2,
        out_specs=(anywhere, anywhere, scalar),
        scratch_shapes=[
            pltpu.VMEM((blocks * comp * comp * tiles, LANES), f32),
            pltpu.VMEM((blocks, rows), jnp.int32),
            pltpu.VMEM((8 * tiles, LANES), jnp.int32),
            pltpu.VMEM(plane, f32),
            pltpu.VMEM((STEPS + 1,) + plane, f32),
            pltpu.VMEM((STEPS + 1, 2) + plane, f32),
            pltpu.VMEM((blocks, tiles, LANES), jnp.int32),
            pltpu.VMEM((blocks, tiles, LANES), jnp.int32),
            pltpu.VMEM((STEPS, 2, tiles, LANES), f32),
            pltpu.VMEM(plane, f32),
            pltpu.VMEM(plane, f32),
            pltpu.VMEM((near, 1, LANES), f32),
            pltpu.VMEM((far, 1, LANES), f32),
            dma((blocks,)),
            dma((3,)),
            dma((2,)),
            dma((STEPS + 1, 2)),
            dma((STEPS + 1, 2)),
            dma((max(near - 1, 1),)),
            dma((near,)),
            dma((max(far - 1, 1),)),
            dma((far,)),
        ],
        compiler_params=pltpu.CompilerParams(collective_id=0, has_side_effects=True),
    )(
        flat(block_values, tiles), block_cols, flat(coarse_rhs, tiles), flat(guess, tiles),
        bound_low, bound_high,
    )
    return unflat(smoothed, comp), unflat(residual, comp), rms


def solution(mesh):
    split = ("sub", "agg")
    return jax.shard_map(
        functools.partial(shards, mesh.shape["sub"], mesh.shape["agg"]),
        mesh=mesh,
        in_specs=(
            P(None, None, None, split),
            P(None, split),
            P(None, split),
            P(None, split),
            P(),
            P(),
        ),
        out_specs=(P(None, split), P(None, split), P()),
        check_vma=False,
    )
```

```python
import functools

import jax
import jax.numpy as jnp
from jax import lax
from jax.experimental import pallas as pl
from jax.experimental.pallas import tpu as pltpu
from jax.sharding import PartitionSpec as P

STEPS = 4
ONE_ROUND = 32
LANES = 128
MESH = pl.DeviceIdType.MESH


def group_size(devices):
    if devices <= ONE_ROUND:
        return devices
    size = 1
    while size * size < devices or devices % size:
        size += 1
    return size


def gather_lanes(rows, index):
    return jnp.take_along_axis(rows, index, axis=1, mode="promise_in_bounds")


def kernel(
    subs, aggs, shape,
    values_hbm, cols_hbm, rhs_hbm, guess_hbm, low_hbm, high_hbm,
    smoothed_hbm, residual_hbm, rms_ref,
    low_ref, high_ref, values, cols, cols_flat, rhs, field, beside, lane_of, tile_of, coef,
    smoothed_out, residual_out, near_sums, far_sums,
    values_sem, load_sem, store_sem, send_sem, recv_sem,
    near_send, near_recv, far_send, far_recv,
):
    blocks, comp, tiles = shape
    devices = subs * aggs
    rows = tiles * LANES
    me = lax.axis_index("sub") * aggs + lax.axis_index("agg")

    def coords(device):
        return (device // aggs, device % aggs)

    following = lax.rem(me + 1, devices)
    previous = lax.rem(me + devices - 1, devices)
    near = group_size(devices)
    far = devices // near
    near_me = lax.rem(me, near)
    near_base = me - near_me
    far_me = me // near
    near_partners = [near_base + lax.rem(near_me + d, near) for d in range(1, near)]
    far_partners = [lax.rem(me + d * near, devices) for d in range(1, far)]

    barrier = pltpu.get_barrier_semaphore()
    partners = [following, previous] + far_partners + near_partners
    for partner in partners:
        pl.semaphore_signal(barrier, inc=1, device_id=coords(partner), device_id_type=MESH)

    load_cols = pltpu.make_async_copy(cols_hbm, cols, load_sem.at[0])
    load_guess = pltpu.make_async_copy(guess_hbm, field.at[0], load_sem.at[1])
    load_rhs = pltpu.make_async_copy(rhs_hbm, rhs, load_sem.at[2])
    load_low = pltpu.make_async_copy(low_hbm, low_ref, load_sem.at[3])
    load_high = pltpu.make_async_copy(high_hbm, high_ref, load_sem.at[4])
    for load in (load_guess, load_cols, load_low, load_high):
        load.start()
    own = [0] + list(range(3, blocks))
    per_block = comp * comp * tiles

    def load_values(k):
        part = pl.ds(k * per_block, per_block)
        return pltpu.make_async_copy(values_hbm.at[part], values.at[part], values_sem.at[k])

    for k in own + [1, 2]:
        load_values(k).start()
    load_rhs.start()

    load_guess.wait()
    pl.semaphore_wait(barrier, len(partners))

    def send(step, source, way):
        return pltpu.make_async_remote_copy(
            src_ref=source,
            dst_ref=beside.at[step, way],
            send_sem=send_sem.at[step, way],
            recv_sem=recv_sem.at[step, way],
            device_id=coords(lax.rem(me + 1 + way * (devices - 2), devices)),
            device_id_type=MESH,
        )

    for way in range(2):
        send(0, field.at[0], way).start()

    load_low.wait()
    load_high.wait()
    low = jnp.full((tiles, LANES), low_ref[0], jnp.int32).astype(jnp.float32) / 4.0
    high = jnp.full((tiles, LANES), high_ref[0], jnp.int32).astype(jnp.float32) / 4.0
    centre = (high + low) / 2.0
    half = (high - low) / 2.0
    spread = centre / half
    ratio = 1.0 / spread
    coef[0, 0] = jnp.zeros((tiles, LANES), jnp.float32)
    coef[0, 1] = 1.0 / centre
    for t in range(1, STEPS):
        ahead = 1.0 / (2.0 * spread - ratio)
        coef[t, 0] = ahead * ratio
        coef[t, 1] = 2.0 * ahead / half
        ratio = ahead

    load_cols.wait()
    for c in range(tiles):
        cols_flat[pl.ds(c * 8, blocks), :] = cols[:, c * LANES:(c + 1) * LANES]
    for k in range(1, blocks):
        plane = {1: previous, 2: following}.get(k, me)
        local = cols_flat[pl.ds(k, tiles, stride=8), :] - plane * rows
        lane_of[k] = local & (LANES - 1)
        tile_of[k] = local >> 7

    def taken(source, k):
        lanes, tile = lane_of[k], tile_of[k]
        out = [None] * comp
        for r in range(tiles):
            here = tile == r
            for j in range(comp):
                row = jnp.broadcast_to(source[pl.ds(r * comp + j, 1), :], (tiles, LANES))
                got = gather_lanes(row, lanes)
                out[j] = got if r == 0 else jnp.where(here, got, out[j])
        return out

    def combine(k, got, total):
        total = list(total)
        for i in range(comp):
            base = (k * comp + i) * comp * tiles
            for j in range(comp):
                total[i] = total[i] - values[pl.ds(base + j, tiles, stride=comp), :] * got[j]
        return total

    def own_part(t, residual):
        source = field.at[t]
        direct = [source[pl.ds(j, tiles, stride=comp), :] for j in range(comp)]
        residual = combine(0, direct, residual)
        for k in own[1:]:
            residual = combine(k, taken(source, k), residual)
        return direct, residual

    def far_part(t, residual):
        even = 1 - lax.rem(me, 2)
        for way in (even, 1 - even):
            send(t, field.at[t], way).wait_recv()
            residual = combine(1 + way, taken(beside.at[t, way], 1 + way), residual)
        return residual

    load_rhs.wait()
    for k in own + [1, 2]:
        load_values(k).wait()

    def step(t, carry):
        smoothed, residual = carry
        direct, residual = own_part(t, residual)
        smoothed = [s + d for s, d in zip(smoothed, direct)]
        residual = far_part(t, residual)
        for j in range(comp):
            field[t + 1, pl.ds(j, tiles, stride=comp), :] = (
                coef[t, 0] * direct[j] + coef[t, 1] * residual[j]
            )
        for way in range(2):
            send(t + 1, field.at[t + 1], way).start()
        return smoothed, residual

    smoothed = [jnp.zeros((tiles, LANES), jnp.float32) for j in range(comp)]
    residual = [rhs[pl.ds(j, tiles, stride=comp), :] for j in range(comp)]
    smoothed, residual = lax.fori_loop(0, STEPS, step, (smoothed, residual))

    direct, residual = own_part(STEPS, residual)
    for j in range(comp):
        smoothed_out[pl.ds(j, tiles, stride=comp), :] = smoothed[j] + direct[j]
    store_smoothed = pltpu.make_async_copy(smoothed_out, smoothed_hbm, store_sem.at[0])
    store_smoothed.start()
    residual = far_part(STEPS, residual)

    squares = residual[0] * residual[0]
    for j in range(1, comp):
        squares = squares + residual[j] * residual[j]
    partial = jnp.sum(squares, axis=0, keepdims=True)

    def spread_sums(sums, slot, partner, send_sems, recv_sems, d):
        return pltpu.make_async_remote_copy(
            src_ref=sums.at[slot],
            dst_ref=sums.at[slot],
            send_sem=send_sems.at[d],
            recv_sem=recv_sems.at[slot],
            device_id=coords(partner),
            device_id_type=MESH,
        )

    def total_over(partial, sums, size, place, partners, send_sems, recv_sems):
        sums[place] = partial
        for d, partner in enumerate(partners):
            spread_sums(sums, place, partner, send_sems, recv_sems, d).start()

        def finish():
            for d, partner in enumerate(partners):
                slot = lax.rem(place + d + 1, size)
                spread_sums(sums, slot, partner, send_sems, recv_sems, d).wait_recv()
            total = sums[0]
            for slot in range(1, size):
                total = total + sums[slot]
            return total

        return finish

    finish = total_over(partial, near_sums, near, near_me, near_partners, near_send, near_recv)
    for j in range(comp):
        residual_out[pl.ds(j, tiles, stride=comp), :] = residual[j]
    store_residual = pltpu.make_async_copy(residual_out, residual_hbm, store_sem.at[1])
    store_residual.start()
    total = finish()
    if far > 1:
        total = total_over(total, far_sums, far, far_me, far_partners, far_send, far_recv)()
    count = float(comp * rows * devices)
    rms = jnp.sqrt(jnp.sum(total, axis=1, keepdims=True) / count + 1e-06)
    rms_ref[0] = rms[0, 0]

    for t in range(STEPS + 1):
        for way in range(2):
            send(t, field.at[t], way).wait_send()
    for d, partner in enumerate(near_partners):
        spread_sums(near_sums, near_me, partner, near_send, near_recv, d).wait_send()
    for d, partner in enumerate(far_partners):
        spread_sums(far_sums, far_me, partner, far_send, far_recv, d).wait_send()
    store_smoothed.wait()
    store_residual.wait()


def flat(field, tiles):
    comp = field.shape[-2]
    lead = field.shape[:-2]
    cut = field.reshape(lead + (comp, tiles, LANES))
    return jnp.swapaxes(cut, -3, -2).reshape(-1, LANES)


def unflat(field, comp):
    tiles = field.shape[0] // comp
    return jnp.swapaxes(field.reshape(tiles, comp, LANES), 0, 1).reshape(comp, tiles * LANES)


def shards(subs, aggs, block_values, block_cols, coarse_rhs, guess, bound_low, bound_high):
    blocks, comp, _, rows = block_values.shape
    tiles = rows // LANES
    devices = subs * aggs
    near = group_size(devices)
    far = devices // near
    f32 = jnp.float32
    plane = (tiles * comp, LANES)
    anywhere = pl.BlockSpec(memory_space=pl.ANY)
    in_hbm = pl.BlockSpec(memory_space=pltpu.HBM)
    scalar = pl.BlockSpec(memory_space=pltpu.SMEM)
    dma = pltpu.SemaphoreType.DMA
    smoothed, residual, rms = pl.pallas_call(
        functools.partial(kernel, subs, aggs, (blocks, comp, tiles)),
        out_shape=(
            jax.ShapeDtypeStruct(plane, f32),
            jax.ShapeDtypeStruct(plane, f32),
            jax.ShapeDtypeStruct((1,), f32),
        ),
        in_specs=[in_hbm] * 6,
        out_specs=(anywhere, anywhere, scalar),
        scratch_shapes=[
            pltpu.SMEM((1,), jnp.int32),
            pltpu.SMEM((1,), jnp.int32),
            pltpu.VMEM((blocks * comp * comp * tiles, LANES), f32),
            pltpu.VMEM((blocks, rows), jnp.int32),
            pltpu.VMEM((8 * tiles, LANES), jnp.int32),
            pltpu.VMEM(plane, f32),
            pltpu.VMEM((STEPS + 1,) + plane, f32),
            pltpu.VMEM((STEPS + 1, 2) + plane, f32),
            pltpu.VMEM((blocks, tiles, LANES), jnp.int32),
            pltpu.VMEM((blocks, tiles, LANES), jnp.int32),
            pltpu.VMEM((STEPS, 2, tiles, LANES), f32),
            pltpu.VMEM(plane, f32),
            pltpu.VMEM(plane, f32),
            pltpu.VMEM((near, 1, LANES), f32),
            pltpu.VMEM((far, 1, LANES), f32),
            dma((blocks,)),
            dma((5,)),
            dma((2,)),
            dma((STEPS + 1, 2)),
            dma((STEPS + 1, 2)),
            dma((max(near - 1, 1),)),
            dma((near,)),
            dma((max(far - 1, 1),)),
            dma((far,)),
        ],
        compiler_params=pltpu.CompilerParams(collective_id=0, has_side_effects=True),
    )(
        flat(block_values, tiles), block_cols, flat(coarse_rhs, tiles), flat(guess, tiles),
        bound_low, bound_high,
    )
    return unflat(smoothed, comp), unflat(residual, comp), rms


def solution(mesh):
    split = ("sub", "agg")
    return jax.shard_map(
        functools.partial(shards, mesh.shape["sub"], mesh.shape["agg"]),
        mesh=mesh,
        in_specs=(
            P(None, None, None, split),
            P(None, split),
            P(None, split),
            P(None, split),
            P(),
            P(),
        ),
        out_specs=(P(None, split), P(None, split), P()),
        check_vma=False,
    )
```

```python
import functools

import jax
import jax.numpy as jnp
from jax import lax
from jax.experimental import pallas as pl
from jax.experimental.pallas import tpu as pltpu
from jax.sharding import PartitionSpec as P

STEPS = 4
ONE_ROUND = 32
LANES = 128
MESH = pl.DeviceIdType.MESH


def group_size(devices):
    if devices <= ONE_ROUND:
        return devices
    size = 1
    while size * size < devices or devices % size:
        size += 1
    return size


def gather_lanes(rows, index):
    return jnp.take_along_axis(rows, index, axis=1, mode="promise_in_bounds")


def kernel(
    subs, aggs, shape,
    values_hbm, cols_hbm, rhs_hbm, guess_hbm, low_hbm, high_hbm,
    smoothed_out, residual_out, rms_ref,
    low_ref, high_ref, values, cols, cols_flat, rhs, field, beside, lane_of, tile_of, coef,
    near_sums, far_sums,
    values_sem, load_sem, send_sem, recv_sem,
    near_send, near_recv, far_send, far_recv,
):
    blocks, comp, tiles = shape
    devices = subs * aggs
    rows = tiles * LANES
    me = lax.axis_index("sub") * aggs + lax.axis_index("agg")

    def coords(device):
        return (device // aggs, device % aggs)

    following = lax.rem(me + 1, devices)
    previous = lax.rem(me + devices - 1, devices)
    near = group_size(devices)
    far = devices // near
    near_me = lax.rem(me, near)
    near_base = me - near_me
    far_me = me // near
    near_partners = [near_base + lax.rem(near_me + d, near) for d in range(1, near)]
    far_partners = [lax.rem(me + d * near, devices) for d in range(1, far)]

    barrier = pltpu.get_barrier_semaphore()
    partners = [following, previous] + far_partners + near_partners
    for partner in partners:
        pl.semaphore_signal(barrier, inc=1, device_id=coords(partner), device_id_type=MESH)

    load_cols = pltpu.make_async_copy(cols_hbm, cols, load_sem.at[0])
    load_guess = pltpu.make_async_copy(guess_hbm, field.at[0], load_sem.at[1])
    load_rhs = pltpu.make_async_copy(rhs_hbm, rhs, load_sem.at[2])
    load_low = pltpu.make_async_copy(low_hbm, low_ref, load_sem.at[3])
    load_high = pltpu.make_async_copy(high_hbm, high_ref, load_sem.at[4])
    for load in (load_guess, load_cols, load_low, load_high):
        load.start()
    own = [0] + list(range(3, blocks))
    per_block = comp * comp * tiles

    def load_values(k):
        part = pl.ds(k * per_block, per_block)
        return pltpu.make_async_copy(values_hbm.at[part], values.at[part], values_sem.at[k])

    for k in own + [1, 2]:
        load_values(k).start()
    load_rhs.start()

    load_guess.wait()
    pl.semaphore_wait(barrier, len(partners))

    def send(step, source, way):
        return pltpu.make_async_remote_copy(
            src_ref=source,
            dst_ref=beside.at[step, way],
            send_sem=send_sem.at[step, way],
            recv_sem=recv_sem.at[step, way],
            device_id=coords(lax.rem(me + 1 + way * (devices - 2), devices)),
            device_id_type=MESH,
        )

    for way in range(2):
        send(0, field.at[0], way).start()

    load_low.wait()
    load_high.wait()
    low = jnp.full((tiles, LANES), low_ref[0], jnp.int32).astype(jnp.float32) / 4.0
    high = jnp.full((tiles, LANES), high_ref[0], jnp.int32).astype(jnp.float32) / 4.0
    centre = (high + low) / 2.0
    half = (high - low) / 2.0
    spread = centre / half
    ratio = 1.0 / spread
    coef[0, 0] = jnp.zeros((tiles, LANES), jnp.float32)
    coef[0, 1] = 1.0 / centre
    for t in range(1, STEPS):
        ahead = 1.0 / (2.0 * spread - ratio)
        coef[t, 0] = ahead * ratio
        coef[t, 1] = 2.0 * ahead / half
        ratio = ahead

    load_cols.wait()
    for c in range(tiles):
        cols_flat[pl.ds(c * 8, blocks), :] = cols[:, c * LANES:(c + 1) * LANES]
    for k in range(1, blocks):
        plane = {1: previous, 2: following}.get(k, me)
        local = cols_flat[pl.ds(k, tiles, stride=8), :] - plane * rows
        lane_of[k] = local & (LANES - 1)
        tile_of[k] = local >> 7

    def taken(source, k):
        lanes, tile = lane_of[k], tile_of[k]
        out = [None] * comp
        for r in range(tiles):
            here = tile == r
            for j in range(comp):
                row = jnp.broadcast_to(source[pl.ds(r * comp + j, 1), :], (tiles, LANES))
                got = gather_lanes(row, lanes)
                out[j] = got if r == 0 else jnp.where(here, got, out[j])
        return out

    def combine(k, got, total):
        total = list(total)
        for i in range(comp):
            base = (k * comp + i) * comp * tiles
            for j in range(comp):
                total[i] = total[i] - values[pl.ds(base + j, tiles, stride=comp), :] * got[j]
        return total

    def own_part(t, residual):
        source = field.at[t]
        direct = [source[pl.ds(j, tiles, stride=comp), :] for j in range(comp)]
        residual = combine(0, direct, residual)
        for k in own[1:]:
            residual = combine(k, taken(source, k), residual)
        return direct, residual

    def far_part(t, residual):
        even = 1 - lax.rem(me, 2)
        for way in (even, 1 - even):
            send(t, field.at[t], way).wait_recv()
            residual = combine(1 + way, taken(beside.at[t, way], 1 + way), residual)
        return residual

    load_rhs.wait()
    for k in own + [1, 2]:
        load_values(k).wait()

    def step(t, carry):
        smoothed, residual = carry
        direct, residual = own_part(t, residual)
        smoothed = [s + d for s, d in zip(smoothed, direct)]
        residual = far_part(t, residual)
        for j in range(comp):
            field[t + 1, pl.ds(j, tiles, stride=comp), :] = (
                coef[t, 0] * direct[j] + coef[t, 1] * residual[j]
            )
        for way in range(2):
            send(t + 1, field.at[t + 1], way).start()
        return smoothed, residual

    smoothed = [jnp.zeros((tiles, LANES), jnp.float32) for j in range(comp)]
    residual = [rhs[pl.ds(j, tiles, stride=comp), :] for j in range(comp)]
    smoothed, residual = lax.fori_loop(0, STEPS, step, (smoothed, residual))

    direct, residual = own_part(STEPS, residual)
    for j in range(comp):
        smoothed_out[pl.ds(j, tiles, stride=comp), :] = smoothed[j] + direct[j]
    residual = far_part(STEPS, residual)

    squares = residual[0] * residual[0]
    for j in range(1, comp):
        squares = squares + residual[j] * residual[j]
    partial = jnp.sum(squares, axis=0, keepdims=True)

    def spread_sums(sums, slot, partner, send_sems, recv_sems, d):
        return pltpu.make_async_remote_copy(
            src_ref=sums.at[slot],
            dst_ref=sums.at[slot],
            send_sem=send_sems.at[d],
            recv_sem=recv_sems.at[slot],
            device_id=coords(partner),
            device_id_type=MESH,
        )

    def total_over(partial, sums, size, place, partners, send_sems, recv_sems):
        sums[place] = partial
        for d, partner in enumerate(partners):
            spread_sums(sums, place, partner, send_sems, recv_sems, d).start()

        def finish():
            for d, partner in enumerate(partners):
                slot = lax.rem(place + d + 1, size)
                spread_sums(sums, slot, partner, send_sems, recv_sems, d).wait_recv()
            total = sums[0]
            for slot in range(1, size):
                total = total + sums[slot]
            return total

        return finish

    finish = total_over(partial, near_sums, near, near_me, near_partners, near_send, near_recv)
    for j in range(comp):
        residual_out[pl.ds(j, tiles, stride=comp), :] = residual[j]
    total = finish()
    if far > 1:
        total = total_over(total, far_sums, far, far_me, far_partners, far_send, far_recv)()
    count = float(comp * rows * devices)
    rms = jnp.sqrt(jnp.sum(total, axis=1, keepdims=True) / count + 1e-06)
    rms_ref[0] = rms[0, 0]

    for t in range(STEPS + 1):
        for way in range(2):
            send(t, field.at[t], way).wait_send()
    for d, partner in enumerate(near_partners):
        spread_sums(near_sums, near_me, partner, near_send, near_recv, d).wait_send()
    for d, partner in enumerate(far_partners):
        spread_sums(far_sums, far_me, partner, far_send, far_recv, d).wait_send()


def flat(field, tiles):
    comp = field.shape[-2]
    lead = field.shape[:-2]
    cut = field.reshape(lead + (comp, tiles, LANES))
    return jnp.swapaxes(cut, -3, -2).reshape(-1, LANES)


def unflat(field, comp):
    tiles = field.shape[0] // comp
    return jnp.swapaxes(field.reshape(tiles, comp, LANES), 0, 1).reshape(comp, tiles * LANES)


def shards(subs, aggs, block_values, block_cols, coarse_rhs, guess, bound_low, bound_high):
    blocks, comp, _, rows = block_values.shape
    tiles = rows // LANES
    devices = subs * aggs
    near = group_size(devices)
    far = devices // near
    f32 = jnp.float32
    plane = (tiles * comp, LANES)
    in_vmem = pl.BlockSpec(memory_space=pltpu.VMEM)
    in_hbm = pl.BlockSpec(memory_space=pltpu.HBM)
    scalar = pl.BlockSpec(memory_space=pltpu.SMEM)
    dma = pltpu.SemaphoreType.DMA
    smoothed, residual, rms = pl.pallas_call(
        functools.partial(kernel, subs, aggs, (blocks, comp, tiles)),
        out_shape=(
            jax.ShapeDtypeStruct(plane, f32),
            jax.ShapeDtypeStruct(plane, f32),
            jax.ShapeDtypeStruct((1,), f32),
        ),
        in_specs=[in_hbm] * 6,
        out_specs=(in_vmem, in_vmem, scalar),
        scratch_shapes=[
            pltpu.SMEM((1,), jnp.int32),
            pltpu.SMEM((1,), jnp.int32),
            pltpu.VMEM((blocks * comp * comp * tiles, LANES), f32),
            pltpu.VMEM((blocks, rows), jnp.int32),
            pltpu.VMEM((8 * tiles, LANES), jnp.int32),
            pltpu.VMEM(plane, f32),
            pltpu.VMEM((STEPS + 1,) + plane, f32),
            pltpu.VMEM((STEPS + 1, 2) + plane, f32),
            pltpu.VMEM((blocks, tiles, LANES), jnp.int32),
            pltpu.VMEM((blocks, tiles, LANES), jnp.int32),
            pltpu.VMEM((STEPS, 2, tiles, LANES), f32),
            pltpu.VMEM((near, 1, LANES), f32),
            pltpu.VMEM((far, 1, LANES), f32),
            dma((blocks,)),
            dma((5,)),
            dma((STEPS + 1, 2)),
            dma((STEPS + 1, 2)),
            dma((max(near - 1, 1),)),
            dma((near,)),
            dma((max(far - 1, 1),)),
            dma((far,)),
        ],
        compiler_params=pltpu.CompilerParams(collective_id=0, has_side_effects=True, vmem_limit_bytes=8 * 1024 * 1024),
    )(
        *[
            pltpu.with_memory_space_constraint(x, pltpu.HBM)
            for x in (
                flat(block_values, tiles), block_cols, flat(coarse_rhs, tiles), flat(guess, tiles),
            )
        ],
        bound_low, bound_high,
    )
    return unflat(smoothed, comp), unflat(residual, comp), rms


def solution(mesh):
    split = ("sub", "agg")
    return jax.shard_map(
        functools.partial(shards, mesh.shape["sub"], mesh.shape["agg"]),
        mesh=mesh,
        in_specs=(
            P(None, None, None, split),
            P(None, split),
            P(None, split),
            P(None, split),
            P(),
            P(),
        ),
        out_specs=(P(None, split), P(None, split), P()),
        check_vma=False,
    )
```

```python
import functools

import jax
import jax.numpy as jnp
from jax import lax
from jax.experimental import pallas as pl
from jax.experimental.pallas import tpu as pltpu
from jax.sharding import PartitionSpec as P

STEPS = 4
ONE_ROUND = 32
LANES = 128
MESH = pl.DeviceIdType.MESH


def gather_lanes(rows, index):
    return jnp.take_along_axis(rows, index, axis=1, mode="promise_in_bounds")


def kernel(
    subs, aggs, shape,
    values_hbm, cols_hbm, rhs_hbm, guess_hbm, low_ref, high_ref,
    smoothed_out, residual_out, rms_ref,
    values, cols, cols_flat, rhs, field, beside, lane_of, tile_of, coef,
    near_sums, far_sums,
    values_sem, load_sem, send_sem, recv_sem,
    near_send, near_recv, far_send, far_recv,
):
    blocks, comp, tiles = shape
    devices = subs * aggs
    rows = tiles * LANES
    load_cols = pltpu.make_async_copy(cols_hbm, cols, load_sem.at[0])
    load_guess = pltpu.make_async_copy(guess_hbm, field.at[0], load_sem.at[1])
    load_rhs = pltpu.make_async_copy(rhs_hbm, rhs, load_sem.at[2])
    for load in (load_guess, load_cols):
        load.start()
    own = [0] + list(range(3, blocks))
    per_block = comp * comp * tiles

    def load_values(k):
        part = pl.ds(k * per_block, per_block)
        return pltpu.make_async_copy(values_hbm.at[part], values.at[part], values_sem.at[k])

    for k in own + [1, 2]:
        load_values(k).start()
    load_rhs.start()

    sub, agg = lax.axis_index("sub"), lax.axis_index("agg")
    me = sub * aggs + agg

    def ahead_of(place, by, size):
        to = place + by
        return jnp.where(to >= size, to - size, to)

    def beside_me(by_sub, by_agg):
        return (ahead_of(sub, by_sub, subs), ahead_of(agg, by_agg, aggs))

    def ring(way):
        turn = jnp.where(way == 0, agg == aggs - 1, agg == 0)
        to_sub = jnp.where(way == 0, ahead_of(sub, 1, subs), ahead_of(sub, subs - 1, subs))
        to_agg = jnp.where(way == 0, ahead_of(agg, 1, aggs), ahead_of(agg, aggs - 1, aggs))
        return (jnp.where(turn, to_sub, sub), to_agg)

    following = ahead_of(me, 1, devices)
    previous = ahead_of(me, devices - 1, devices)
    one_round = devices <= ONE_ROUND
    if one_round:
        near_steps = [(a, b) for a in range(subs) for b in range(aggs)][1:]
        near_steps = near_steps[::-1]
        near, near_me = devices, me
        far_steps = []
    else:
        near_steps = [(0, b) for b in range(1, aggs)]
        near, near_me = aggs, agg
        far_steps = [(a, 0) for a in range(1, subs)]
    near_partners = [beside_me(a, b) for a, b in near_steps]
    far_partners = [beside_me(a, b) for a, b in far_steps]

    barrier = pltpu.get_barrier_semaphore()
    partners = far_partners + near_partners
    if not one_round:
        partners = [ring(0), ring(1)] + partners
    for partner in partners:
        pl.semaphore_signal(barrier, inc=1, device_id=partner, device_id_type=MESH)

    load_guess.wait()
    pl.semaphore_wait(barrier, len(partners))

    def send(step, source, way):
        return pltpu.make_async_remote_copy(
            src_ref=source,
            dst_ref=beside.at[step, way],
            send_sem=send_sem.at[step, way],
            recv_sem=recv_sem.at[step, way],
            device_id=ring(way),
            device_id_type=MESH,
        )

    for way in range(2):
        send(0, field.at[0], way).start()

    low = jnp.full((tiles, LANES), low_ref[0], jnp.int32).astype(jnp.float32) / 4.0
    high = jnp.full((tiles, LANES), high_ref[0], jnp.int32).astype(jnp.float32) / 4.0
    centre = (high + low) / 2.0
    half = (high - low) / 2.0
    spread = centre / half
    ratio = 1.0 / spread
    coef[0, 0] = jnp.zeros((tiles, LANES), jnp.float32)
    coef[0, 1] = 1.0 / centre
    for t in range(1, STEPS):
        ahead = 1.0 / (2.0 * spread - ratio)
        coef[t, 0] = ahead * ratio
        coef[t, 1] = 2.0 * ahead / half
        ratio = ahead

    load_cols.wait()
    for c in range(tiles):
        cols_flat[pl.ds(c * 8, blocks), :] = cols[:, c * LANES:(c + 1) * LANES]
    for k in range(1, blocks):
        plane = {1: previous, 2: following}.get(k, me)
        local = cols_flat[pl.ds(k, tiles, stride=8), :] - plane * rows
        lane_of[k] = local & (LANES - 1)
        tile_of[k] = local >> 7

    def taken(source, k):
        lanes, tile = lane_of[k], tile_of[k]
        out = [None] * comp
        for r in range(tiles):
            here = tile == r
            for j in range(comp):
                row = jnp.broadcast_to(source[pl.ds(r * comp + j, 1), :], (tiles, LANES))
                got = gather_lanes(row, lanes)
                out[j] = got if r == 0 else jnp.where(here, got, out[j])
        return out

    def combine(k, got, total):
        total = list(total)
        for i in range(comp):
            base = (k * comp + i) * comp * tiles
            for j in range(comp):
                total[i] = total[i] - values[pl.ds(base + j, tiles, stride=comp), :] * got[j]
        return total

    def own_part(t, residual):
        source = field.at[t]
        direct = [source[pl.ds(j, tiles, stride=comp), :] for j in range(comp)]
        residual = combine(0, direct, residual)
        for k in own[1:]:
            residual = combine(k, taken(source, k), residual)
        return direct, residual

    def far_part(t, residual):
        even = 1 - lax.rem(me, 2)
        for way in (even, 1 - even):
            send(t, field.at[t], way).wait_recv()
            residual = combine(1 + way, taken(beside.at[t, way], 1 + way), residual)
        return residual

    load_rhs.wait()
    for k in own + [1, 2]:
        load_values(k).wait()

    def step(t, carry):
        smoothed, residual = carry
        direct, residual = own_part(t, residual)
        smoothed = [s + d for s, d in zip(smoothed, direct)]
        residual = far_part(t, residual)
        for j in range(comp):
            field[t + 1, pl.ds(j, tiles, stride=comp), :] = (
                coef[t, 0] * direct[j] + coef[t, 1] * residual[j]
            )
        for way in range(2):
            send(t + 1, field.at[t + 1], way).start()
        return smoothed, residual

    smoothed = [jnp.zeros((tiles, LANES), jnp.float32) for j in range(comp)]
    residual = [rhs[pl.ds(j, tiles, stride=comp), :] for j in range(comp)]
    smoothed, residual = lax.fori_loop(0, STEPS, step, (smoothed, residual))

    direct, residual = own_part(STEPS, residual)
    for j in range(comp):
        smoothed_out[pl.ds(j, tiles, stride=comp), :] = smoothed[j] + direct[j]
    residual = far_part(STEPS, residual)

    squares = residual[0] * residual[0]
    for j in range(1, comp):
        squares = squares + residual[j] * residual[j]
    partial = jnp.sum(squares, axis=0, keepdims=True)

    def spread_sums(sums, slot, partner, send_sems, recv_sems, d):
        return pltpu.make_async_remote_copy(
            src_ref=sums.at[slot],
            dst_ref=sums.at[slot],
            send_sem=send_sems.at[d],
            recv_sem=recv_sems.at[slot],
            device_id=partner,
            device_id_type=MESH,
        )

    def slot_of(partner):
        return partner[0] * aggs + partner[1] if one_round else partner[1]

    near_sums[near_me] = partial
    for d, partner in enumerate(near_partners):
        spread_sums(near_sums, near_me, partner, near_send, near_recv, d).start()
    for j in range(comp):
        residual_out[pl.ds(j, tiles, stride=comp), :] = residual[j]
    for d, partner in enumerate(near_partners):
        spread_sums(near_sums, slot_of(partner), partner, near_send, near_recv, d).wait_recv()
    total = jnp.sum(near_sums[...], axis=0)
    if far_partners:
        far_sums[sub] = total
        for d, partner in enumerate(far_partners):
            spread_sums(far_sums, sub, partner, far_send, far_recv, d).start()
        for d, partner in enumerate(far_partners):
            spread_sums(far_sums, partner[0], partner, far_send, far_recv, d).wait_recv()
        total = jnp.sum(far_sums[...], axis=0)
    count = float(comp * rows * devices)
    rms_ref[...] = jnp.sqrt(jnp.sum(total, axis=1, keepdims=True) / count + 1e-06)

    for t in range(STEPS + 1):
        for way in range(2):
            send(t, field.at[t], way).wait_send()
    for d, partner in enumerate(near_partners):
        spread_sums(near_sums, near_me, partner, near_send, near_recv, d).wait_send()
    for d, partner in enumerate(far_partners):
        spread_sums(far_sums, sub, partner, far_send, far_recv, d).wait_send()


def put_out(*refs):
    count = len(refs) // 2
    sems = refs[-1]
    copies = [
        pltpu.make_async_copy(refs[i], refs[count + i], sems.at[i]) for i in range(count)
    ]
    for copy in copies:
        copy.start()
    for copy in copies:
        copy.wait()


def flat(field, tiles):
    comp = field.shape[-2]
    lead = field.shape[:-2]
    cut = field.reshape(lead + (comp, tiles, LANES))
    return jnp.swapaxes(cut, -3, -2).reshape(-1, LANES)


def unflat(field, comp):
    tiles = field.shape[0] // comp
    return jnp.swapaxes(field.reshape(tiles, comp, LANES), 0, 1).reshape(comp, tiles * LANES)


def shards(subs, aggs, block_values, block_cols, coarse_rhs, guess, bound_low, bound_high):
    blocks, comp, _, rows = block_values.shape
    tiles = rows // LANES
    devices = subs * aggs
    near, far = (devices, 1) if devices <= ONE_ROUND else (aggs, subs)
    f32 = jnp.float32
    plane = (tiles * comp, LANES)
    anywhere = pl.BlockSpec(memory_space=pl.ANY)
    in_vmem = pl.BlockSpec(memory_space=pltpu.VMEM)
    in_hbm = pl.BlockSpec(memory_space=pltpu.HBM)
    dma = pltpu.SemaphoreType.DMA
    smoothed, residual, rms = pl.pallas_call(
        functools.partial(kernel, subs, aggs, (blocks, comp, tiles)),
        out_shape=(
            jax.ShapeDtypeStruct(plane, f32),
            jax.ShapeDtypeStruct(plane, f32),
            jax.ShapeDtypeStruct((1, 1), f32),
        ),
        in_specs=[in_hbm] * 4 + [pl.BlockSpec(memory_space=pltpu.SMEM)] * 2,
        out_specs=(in_vmem,) * 3,
        scratch_shapes=[
            pltpu.VMEM((blocks * comp * comp * tiles, LANES), f32),
            pltpu.VMEM((blocks, rows), jnp.int32),
            pltpu.VMEM((8 * tiles, LANES), jnp.int32),
            pltpu.VMEM(plane, f32),
            pltpu.VMEM((STEPS + 1,) + plane, f32),
            pltpu.VMEM((STEPS + 1, 2) + plane, f32),
            pltpu.VMEM((blocks, tiles, LANES), jnp.int32),
            pltpu.VMEM((blocks, tiles, LANES), jnp.int32),
            pltpu.VMEM((STEPS, 2, tiles, LANES), f32),
            pltpu.VMEM((near, 1, LANES), f32),
            pltpu.VMEM((far, 1, LANES), f32),
            dma((blocks,)),
            dma((5,)),
            dma((STEPS + 1, 2)),
            dma((STEPS + 1, 2)),
            dma((max(near - 1, 1),)),
            dma((near,)),
            dma((max(far - 1, 1),)),
            dma((far,)),
        ],
        compiler_params=pltpu.CompilerParams(collective_id=0, has_side_effects=True, vmem_limit_bytes=8 * 1024 * 1024),
    )(
        *[
            pltpu.with_memory_space_constraint(x, pltpu.HBM)
            for x in (
                flat(block_values, tiles), block_cols, flat(coarse_rhs, tiles), flat(guess, tiles),
            )
        ],
        bound_low, bound_high,
    )
    smoothed, residual, rms = pl.pallas_call(
        put_out,
        out_shape=(
            jax.ShapeDtypeStruct(plane, f32),
            jax.ShapeDtypeStruct(plane, f32),
            jax.ShapeDtypeStruct((1, 1), f32),
        ),
        in_specs=[anywhere] * 3,
        out_specs=(anywhere,) * 3,
        scratch_shapes=[dma((3,))],
        compiler_params=pltpu.CompilerParams(vmem_limit_bytes=8 * 1024 * 1024),
    )(smoothed, residual, rms)
    return unflat(smoothed, comp), unflat(residual, comp), rms.reshape(1)


def solution(mesh):
    split = ("sub", "agg")
    return jax.shard_map(
        functools.partial(shards, mesh.shape["sub"], mesh.shape["agg"]),
        mesh=mesh,
        in_specs=(
            P(None, None, None, split),
            P(None, split),
            P(None, split),
            P(None, split),
            P(),
            P(),
        ),
        out_specs=(P(None, split), P(None, split), P()),
        check_vma=False,
    )
```
